256 devices in a mesh: dev: 64 (over z, y, core), rep: 4 (over x).
Axes of the slice: x: 4, y: 4, z: 8, core: 2. Of those that a mesh axis runs over, the one named last changes fastest.
Arguments:
- features: bfloat16 [262144, 256], P(('dev', 'rep')), may hold values from -6 to 6
- history: bfloat16 [262144, 256], P(('dev', 'rep')), may hold values from -6 to 6
- new_owner: int32 [256, 64], P(('dev', 'rep')), may hold values from 0 to 63, as said below
- pull_rows: int32 [262144], P(('dev', 'rep')), may hold values from 0 to 1023
- occupancy: int32 [2048, 16], P(('dev', 'rep')), may hold values from 0 to 1, as said below
- adj_local: bfloat16 [262144, 1024], P(('dev', 'rep')), may hold values from -0.125 to 0.125
- adj_boundary: bfloat16 [262144, 1024], P(('dev', 'rep')), may hold values from -0.125 to 0.125
- w_first: bfloat16 [256, 256], replicated, may hold values from -0.375 to 0.375
- bias_first: float32 [256], replicated, may hold values from -3 to 3
- w_second: bfloat16 [256, 256], replicated, may hold values from -0.375 to 0.375
- cotangent: bfloat16 [262144, 256], P(('dev', 'rep')), may hold values from -24 to 24
Outputs:
- hidden: bfloat16 [262144, 256], P(('dev', 'rep'))
- output: bfloat16 [262144, 256], P(('dev', 'rep'))
- w_second_grad: float32 [256, 256], replicated
The draws below stay inside these ranges and needn't reach their ends.
Inputs may be any that keep to these rules, and one draw needn't show every extreme that they name: Each row of new_owner is a permutation of 0 to 63. `occupancy`: tile flags of 0 or 1.
All inputs are finite; a program needn't handle non-finite values.
Results may differ from the reference program's by a relative error of at most 0.0061.
Values may be sent and summed in bfloat16 or wider, within the bound.
A program may use at most 64 MiB of HBM per device.

```python
import jax
import jax.numpy as jnp
from jax import lax

F = 256
ROWS_DEV = 1024
PULL_DEV = 1024
NODES = 262144
N_DEV = 64
N_REP = 4


def draw_new_owner(key, part):
    keys = jax.random.split(jax.random.fold_in(key, 11), N_DEV * N_REP)

    def shuffle(single):
        return jax.random.permutation(single, N_DEV)
    return jax.vmap(shuffle)(keys).astype(jnp.int32)


def draw_occupancy(key, part):
    tile_rows = ROWS_DEV // 128
    tile_cols = (ROWS_DEV + PULL_DEV) // 128
    total = N_DEV * N_REP
    first, second = jax.random.split(jax.random.fold_in(key, 23))
    level = jax.random.randint(first, (total, 1, 1), 1, 5)
    rolled = jax.random.randint(second, (total, tile_rows, tile_cols), 0, 4)
    return (rolled < level).astype(jnp.int32).reshape(total * tile_rows, tile_cols)


def set_ends(entries, stream_key, smallest, top_value):
    spot = [jax.random.randint(jax.random.fold_in(stream_key, axis), (), 0, length) for axis, length in enumerate(entries.shape)]
    longest = entries.shape.index(max(entries.shape))
    next_to = spot[:longest] + [(spot[longest] + 1) % entries.shape[longest]] + spot[longest + 1:]
    return entries.at[tuple(spot)].set(smallest).at[tuple(next_to)].set(top_value)


def with_spikes(values, rng, source, target, shards_of, factor):
    def block_of(dim):
        return (jnp.arange(values.shape[dim]) // (values.shape[dim] // shards_of)).reshape((-1,) + (1,) * (values.ndim - 1 - dim))

    first = jax.random.permutation(rng, shards_of)[block_of(target)]
    other_side = (block_of(target) + shards_of // 2) % shards_of
    return jnp.where((block_of(source) == first) | (block_of(source) == other_side), factor * values, values)


def block_scale(stream_key, dims, shards, low, high):
    def one(dim, shards_of):
        draws = jax.random.uniform(jax.random.fold_in(jax.random.fold_in(stream_key, 6), dim), (shards_of,), jnp.float32, low / len(shards), high / len(shards))
        return jnp.repeat(jnp.exp(draws), dims[dim] // shards_of).reshape((-1,) + (1,) * (len(dims) - dim - 1))

    loudness = one(*shards[0])
    for cut in shards[1:]:
        loudness = loudness * one(*cut)
    return loudness


def bell_draw(stream_key, dims, scale, limit, cuts=(), kind=jnp.bfloat16):
    loudness = block_scale(stream_key, dims, cuts, -0.22, 0.18) if cuts else 1.0
    values = jax.random.normal(stream_key, dims, jnp.float32) * scale * loudness
    return jnp.minimum(jnp.maximum(values, -limit), limit).astype(kind)


def gaussian_with(stream_key, extent, scale, bound, cuts, heavy, kind=jnp.bfloat16):
    array = scale * jax.random.normal(stream_key, extent, jnp.float32)
    if cuts:
        array = array * block_scale(stream_key, extent, cuts, -0.22, 0.18)
    return jnp.clip(with_spikes(array, jax.random.fold_in(stream_key, 3), *heavy), -bound, bound).astype(kind)


def setup_inputs(seed: int = 0) -> dict:
    splits = jax.random.split(jax.random.key(seed), 12)
    features = bell_draw(splits[0], (NODES, F), 1.0, 6.0, ((0, 256),))
    history = bell_draw(splits[1], (NODES, F), 1.0, 6.0, ((0, 256),))
    new_owner = draw_new_owner(jax.random.fold_in(splits[11], 71), 0)
    pull_rows = set_ends(jax.random.randint(splits[3], (N_DEV * N_REP * PULL_DEV,), 0, ROWS_DEV), jax.random.fold_in(splits[3], 1), 0, ROWS_DEV - 1).astype(jnp.int32)
    occupancy = draw_occupancy(jax.random.fold_in(splits[11], 71), 0)
    adj_local = bell_draw(splits[5], (NODES, ROWS_DEV), (ROWS_DEV + PULL_DEV) ** -0.5, 0.125, ((0, 256),))
    adj_boundary = bell_draw(splits[6], (NODES, PULL_DEV), (ROWS_DEV + PULL_DEV) ** -0.5, 0.125, ((0, 256),))
    w_first = bell_draw(splits[7], (F, F), F ** -0.5, 0.375)
    bias_first = bell_draw(splits[8], (F,), 0.5, 3.0, (), jnp.float32)
    w_second = bell_draw(splits[9], (F, F), F ** -0.5, 0.375)
    cotangent = gaussian_with(splits[10], (NODES, F), 1.0, 24.0, ((0, 256),), (0, 1, 256, 6.0))
    return dict(features=features, history=history, new_owner=new_owner, pull_rows=pull_rows, occupancy=occupancy, adj_local=adj_local, adj_boundary=adj_boundary, w_first=w_first, bias_first=bias_first, w_second=w_second, cotangent=cotangent)


def expand(occupied):
    return jnp.repeat(jnp.repeat(occupied, 128, axis=-2), 128, axis=-1).astype(jnp.bfloat16)


def reference(features, history, new_owner, pull_rows, occupancy, adj_local, adj_boundary, w_first, bias_first, w_second, cotangent):
    peer_count = N_DEV
    copies = N_REP
    height = ROWS_DEV
    breadth = F
    cluster = height // peer_count
    pulled = PULL_DEV
    per_peer = pulled // peer_count
    indices = jnp.arange(peer_count, dtype=jnp.int32)
    routes = new_owner.reshape(peer_count, copies, peer_count)
    matches = (routes[:, :, :, None] == indices).astype(jnp.int32)
    inverse = jnp.sum(matches * indices[:, None], axis=2).astype(jnp.int32)

    def migrate(values):
        blocks = values.reshape(peer_count, copies, peer_count, cluster, breadth)
        where_from = jnp.broadcast_to(inverse[:, :, :, None, None], blocks.shape)
        arrived = jnp.take_along_axis(blocks, where_from, axis=2)
        return arrived.transpose(2, 1, 0, 3, 4).reshape(peer_count, copies, height, breadth)

    own_x = migrate(features)
    own_h = migrate(history)
    wanted = pull_rows.reshape(peer_count, copies, pulled)
    owners = jnp.arange(pulled, dtype=jnp.int32) // per_peer
    flat_rows = (owners[None, None, :] * height + wanted).astype(jnp.int32)
    replica_ids = jnp.arange(copies, dtype=jnp.int32)[None, :, None]

    def fetch_remote(values):
        spread = values.transpose(1, 0, 2, 3).reshape(copies, peer_count * height, breadth)
        return spread[replica_ids, flat_rows]

    def scatter(partial_value):
        summed = jnp.zeros((copies, peer_count * height, breadth), jnp.float32)
        summed = summed.at[replica_ids, flat_rows].add(partial_value.astype(jnp.float32))
        summed = summed.reshape(copies, peer_count, height, breadth).transpose(1, 0, 2, 3)
        return summed.reshape(peer_count * copies * height, breadth)

    tile_mask = occupancy.reshape(peer_count * copies, height // 128, (height + pulled) // 128)
    local_adj = adj_local.reshape(peer_count * copies, height, height)
    edge_adj = adj_boundary.reshape(peer_count * copies, height, pulled)

    def layer_terms(owned, remote):
        def device(operands):
            owned_rows, theirs, local_tile, edge_tile, flags = operands
            full_mask = expand(flags)
            local_tile = local_tile * full_mask[:, :height]
            edge_tile = edge_tile * full_mask[:, height:]
            summed = jnp.dot(local_tile, owned_rows, preferred_element_type=jnp.float32)
            summed = summed + jnp.dot(edge_tile, theirs, preferred_element_type=jnp.float32)
            partial_value = lax.dot_general(edge_tile, owned_rows, (((0,), (0,)), ((), ())), preferred_element_type=jnp.float32)
            return summed, partial_value.astype(jnp.bfloat16)

        summed, partial_value = lax.map(device, (owned.reshape(-1, height, breadth), remote.reshape(-1, pulled, breadth), local_adj, edge_adj, tile_mask))
        return summed.reshape(-1, breadth), partial_value.reshape(peer_count, copies, pulled, breadth)

    summed_one, partial_one = layer_terms(own_x, fetch_remote(own_x))
    aggregate_one = (summed_one + scatter(partial_one)).astype(jnp.bfloat16)
    hidden = jnp.maximum(jnp.dot(aggregate_one, w_first, preferred_element_type=jnp.float32) + bias_first, 0.0).astype(jnp.bfloat16)
    summed_two, partial_two = layer_terms(hidden.reshape(peer_count, copies, height, breadth), fetch_remote(own_h))
    aggregate_two = (summed_two + scatter(partial_two)).astype(jnp.bfloat16)
    output = jnp.dot(aggregate_two, w_second, preferred_element_type=jnp.float32).astype(jnp.bfloat16)
    gradient = lax.dot_general(aggregate_two, cotangent, (((0,), (0,)), ((), ())), preferred_element_type=jnp.float32)
    return hidden, output, gradient
```

```python
import functools

import jax
import jax.numpy as jnp
from jax import lax
from jax.experimental import pallas as pl
from jax.experimental.pallas import tpu as pltpu
from jax.sharding import PartitionSpec as P

MESH = pl.DeviceIdType.MESH
F32, BF16, I32 = jnp.float32, jnp.bfloat16, jnp.int32

REQ, MIG_X, MIG_H, PULL_X, PUSH_1, PULL_H, PUSH_2, GRAD_A, GRAD_B, GRAD_C = range(10)


def iota(shape, dim):
    return lax.broadcasted_iota(I32, shape, dim)


def ones_where(condition):
    return jnp.where(condition, 1.0, 0.0).astype(BF16)


def dot(a, b):
    return jnp.dot(a, b, preferred_element_type=F32)


def step_kernel(
    n_dev,
    n_rep,
    n_y,
    n_core,
    features,
    history,
    owner_ref,
    pull_ref,
    occ_ref,
    adj_local,
    adj_boundary,
    w_first,
    bias_first,
    w_second,
    cotangent,
    hidden_out,
    output_out,
    grad_out,
    x_in,
    h_in,
    local,
    edge,
    edge_t,
    w1,
    w2,
    cot,
    cot_t,
    send_x,
    send_h,
    own_x,
    own_h,
    asked,
    asked_flat,
    sel,
    sel_t,
    occ_rows,
    fetch_x,
    fetch_h,
    part_1,
    part_2,
    far_x,
    far_h,
    push_1,
    push_2,
    acc,
    hidden,
    agg,
    result,
    grad,
    grad_in,
    slab_sum,
    line_in,
    total,
    grad_all,
    load_sem,
    store_sem,
    send_sem,
    recv_sem,
):
    me, rep = lax.axis_index("dev"), lax.axis_index("rep")
    rows, breadth = x_in.shape
    per_peer = rows // n_dev
    per_z = n_y * n_core
    slab = per_z * n_rep
    n_z = n_dev // per_z
    chunk = breadth // slab
    my_z, my_yc = me // per_z, me % per_z
    my_slab = my_yc * n_rep + rep
    step = 256

    def dev_peer(i):
        return lax.rem(me + i, n_dev)

    def slab_peer(i):
        return lax.rem(my_slab + i, slab)

    def slab_id(q):
        return (my_z * per_z + q // n_rep, q % n_rep)

    def each(count, body):
        def run(i, carry):
            body(i)
            return carry

        lax.fori_loop(1, count, run, 0)

    barrier = pltpu.get_barrier_semaphore()

    def greet(device):
        pl.semaphore_signal(barrier, inc=1, device_id=device, device_id_type=MESH)

    each(n_dev, lambda i: greet((dev_peer(i), rep)))

    def greet_across(i):
        r = lax.rem(rep + i, n_rep)

        def run(j, carry):
            greet((my_z * per_z + j, r))
            return carry

        lax.fori_loop(0, per_z, run, 0)

    each(n_rep, greet_across)

    loads = [
        pltpu.make_async_copy(src, dst, load_sem.at[k])
        for k, (src, dst) in enumerate(
            [
                (features, x_in),
                (history, h_in),
                (adj_local, local),
                (adj_boundary, edge),
                (cotangent, cot),
                (w_first, w1),
                (w_second, w2),
            ]
        )
    ]
    for load in loads:
        load.start()

    owners = jnp.broadcast_to(owner_ref[...], (8, n_dev)).astype(F32).astype(BF16)
    spread = ones_where(iota((n_dev, rows), 0) == iota((n_dev, rows), 1) // per_peer)
    target = dot(owners, spread)[0:1].astype(I32) * per_peer + iota((1, rows), 1) % per_peer
    loads[0].wait()
    loads[1].wait()

    def arrange(i, carry):
        at = pl.ds(pl.multiple_of(i * step, step), step)
        pick = ones_where(iota((step, rows), 0) + i * step == target)
        send_x[at] = dot(pick, x_in[...]).astype(BF16)
        send_h[at] = dot(pick, h_in[...]).astype(BF16)
        return carry

    lax.fori_loop(0, rows // step, arrange, 0)

    def block(d):
        return pl.ds(pl.multiple_of(d * per_peer, per_peer), per_peer)

    own_x[block(me)] = send_x[block(me)]
    own_h[block(me)] = send_h[block(me)]
    asked[me] = pull_ref[me // per_z]

    pl.semaphore_wait(barrier, n_dev - 1 + (n_rep - 1) * per_z)

    def remote(src, dst, stage, device):
        pltpu.make_async_remote_copy(
            src_ref=src,
            dst_ref=dst,
            send_sem=send_sem.at[stage],
            recv_sem=recv_sem.at[stage],
            device_id=device,
            device_id_type=MESH,
        ).start()

    def send_requests(i):
        peer = dev_peer(i)
        remote(pull_ref.at[peer // per_z], asked.at[me], REQ, (peer, rep))

    def exchange(src, dst, stage):
        def one(i):
            peer = dev_peer(i)
            remote(src.at[block(peer)], dst.at[block(me)], stage, (peer, rep))

        each(n_dev, one)

    others = pl.ds(0, rows - per_peer)

    def landed(dst, stage):
        pltpu.make_async_copy(dst.at[others], dst.at[others], recv_sem.at[stage]).wait()

    def left(src, stage):
        pltpu.make_async_copy(src.at[others], src.at[others], send_sem.at[stage]).wait()

    each(n_dev, send_requests)
    exchange(send_x, own_x, MIG_X)
    exchange(send_h, own_h, MIG_H)

    n_tiles = 2 * rows // 128
    tile_of = ones_where(iota((n_tiles, 2 * rows), 0) == iota((n_tiles, 2 * rows), 1) // 128)
    occ_rows[...] = dot(occ_ref[...].astype(F32).astype(BF16), tile_of)
    loads[2].wait()
    loads[3].wait()

    def mask_rows(i, carry):
        at = pl.ds(pl.multiple_of(i * 128, 128), 128)
        there = occ_rows[pl.ds(i, 1), :]
        flags = jnp.broadcast_to(there, (128, 2 * rows)).astype(BF16)
        local[at] = local[at] * flags[:, :rows]
        kept = edge[at] * flags[:, rows:]
        edge[at] = kept
        edge_t[:, at] = kept.T
        return carry

    lax.fori_loop(0, rows // 128, mask_rows, 0)

    pltpu.make_async_copy(
        asked.at[pl.ds(0, n_dev - 1)], asked.at[pl.ds(0, n_dev - 1)], recv_sem.at[REQ]
    ).wait()
    for d in range(n_dev):
        asked_flat[d : d + 1, :] = asked[d]
    first = (me % per_z) * per_peer
    wanted = asked_flat[...]
    high = (wanted // per_peer).astype(F32).astype(BF16)
    low = (wanted % per_peer).astype(F32).astype(BF16)
    widen = ones_where(iota((128, rows), 0) == first + iota((128, rows), 1) % per_peer)
    along = dot(high, widen) * per_peer + dot(low, widen)
    mine = iota((n_dev, rows), 0) == iota((n_dev, rows), 1) // per_peer
    as_row = jnp.sum(jnp.where(mine, along, 0.0), axis=0, keepdims=True).astype(I32)
    all_ones = jnp.ones((128, 128), BF16)

    def select(i, carry):
        at = pl.ds(pl.multiple_of(i * step, step), step)
        sel[at] = ones_where(iota((step, rows), 0) + i * step == as_row)
        entry = iota((step, n_dev), 0) + i * step
        take = ones_where(entry // per_peer == iota((step, n_dev), 1))
        here = iota((step, 128), 1) == first + iota((step, 128), 0) % per_peer
        hi = jnp.where(here, dot(take, high), 0.0).astype(BF16)
        lo = jnp.where(here, dot(take, low), 0.0).astype(BF16)
        as_column = (dot(hi, all_ones) * per_peer + dot(lo, all_ones)).astype(I32)
        for c in range(rows // 128):
            sel_t[at, c * 128 : (c + 1) * 128] = ones_where(as_column == iota((step, 128), 1) + c * 128)
        return carry

    lax.fori_loop(0, rows // step, select, 0)

    def product(dst, a, b):
        def run(i, carry):
            at = pl.ds(pl.multiple_of(i * step, step), step)
            dst[at] = dot(a[at], b[...]).astype(dst.dtype)
            return carry

        lax.fori_loop(0, a.shape[0] // step, run, 0)

    def add_product(dst, a, b):
        def run(i, carry):
            at = pl.ds(pl.multiple_of(i * step, step), step)
            dst[at] += dot(a[at], b[...])
            return carry

        lax.fori_loop(0, a.shape[0] // step, run, 0)

    landed(own_x, MIG_X)
    product(fetch_x, sel_t, own_x)
    exchange(fetch_x, far_x, PULL_X)
    product(part_1, edge_t, own_x)
    exchange(part_1, push_1, PUSH_1)
    far_x[block(me)] = fetch_x[block(me)]
    push_1[block(me)] = part_1[block(me)]
    product(acc, local, own_x)

    landed(own_h, MIG_H)
    product(fetch_h, sel_t, own_h)
    exchange(fetch_h, far_h, PULL_H)
    far_h[block(me)] = fetch_h[block(me)]
    loads[4].wait()
    cot_t[...] = cot[...].T
    loads[5].wait()
    loads[6].wait()

    landed(far_x, PULL_X)
    add_product(acc, edge, far_x)
    landed(push_1, PUSH_1)

    def to_hidden(i, carry):
        at = pl.ds(pl.multiple_of(i * step, step), step)
        gathered = (acc[at] + dot(sel[at], push_1[...])).astype(BF16)
        hidden[at] = jnp.maximum(dot(gathered, w1[...]) + bias_first[...], 0.0).astype(BF16)
        return carry

    lax.fori_loop(0, rows // step, to_hidden, 0)

    product(part_2, edge_t, hidden)
    exchange(part_2, push_2, PUSH_2)
    push_2[block(me)] = part_2[block(me)]
    hidden_store = pltpu.make_async_copy(hidden, hidden_out, store_sem.at[0])
    hidden_store.start()
    product(acc, local, hidden)
    landed(far_h, PULL_H)
    add_product(acc, edge, far_h)
    landed(push_2, PUSH_2)

    def to_agg(i, carry):
        at = pl.ds(pl.multiple_of(i * step, step), step)
        agg[at] = (acc[at] + dot(sel[at], push_2[...])).astype(BF16)
        return carry

    lax.fori_loop(0, rows // step, to_agg, 0)

    grad[...] = dot(cot_t[...], agg[...])

    def part_of(q):
        return pl.ds(pl.multiple_of(q * chunk, chunk), chunk)

    def scatter_grad(i):
        q = slab_peer(i)
        remote(grad.at[part_of(q)], grad_in.at[my_slab], GRAD_A, slab_id(q))

    each(slab, scatter_grad)
    grad_in[my_slab] = grad[part_of(my_slab)]
    product(result, agg, w2)
    output_store = pltpu.make_async_copy(result, output_out, store_sem.at[1])
    output_store.start()
    pltpu.make_async_copy(
        grad_in.at[pl.ds(0, slab - 1)], grad_in.at[pl.ds(0, slab - 1)], recv_sem.at[GRAD_A]
    ).wait()
    slab_sum[...] = jnp.sum(grad_in[...], axis=0)

    def along_z(i):
        z = lax.rem(my_z + i, n_z)
        remote(slab_sum, line_in.at[my_z], GRAD_B, (z * per_z + my_yc, rep))

    each(n_z, along_z)
    line_in[my_z] = slab_sum[...]
    pltpu.make_async_copy(
        line_in.at[pl.ds(0, n_z - 1)], line_in.at[pl.ds(0, n_z - 1)], recv_sem.at[GRAD_B]
    ).wait()
    total[...] = jnp.sum(line_in[...], axis=0)

    def spread_total(i):
        remote(total, grad_all.at[part_of(my_slab)], GRAD_C, slab_id(slab_peer(i)))

    each(slab, spread_total)
    grad_all[part_of(my_slab)] = total[...]
    pltpu.make_async_copy(
        grad_all.at[pl.ds(0, breadth - chunk)],
        grad_all.at[pl.ds(0, breadth - chunk)],
        recv_sem.at[GRAD_C],
    ).wait()
    grad_store = pltpu.make_async_copy(grad_all, grad_out, store_sem.at[2])
    grad_store.start()

    pltpu.make_async_copy(
        asked.at[pl.ds(0, n_dev - 1)], asked.at[pl.ds(0, n_dev - 1)], send_sem.at[REQ]
    ).wait()
    left(send_x, MIG_X)
    left(send_h, MIG_H)
    left(fetch_x, PULL_X)
    left(part_1, PUSH_1)
    left(fetch_h, PULL_H)
    left(part_2, PUSH_2)
    for stage in (GRAD_A, GRAD_C):
        pltpu.make_async_copy(
            grad.at[pl.ds(0, breadth - chunk)],
            grad.at[pl.ds(0, breadth - chunk)],
            send_sem.at[stage],
        ).wait()
    pltpu.make_async_copy(
        line_in.at[pl.ds(0, n_z - 1)], line_in.at[pl.ds(0, n_z - 1)], send_sem.at[GRAD_B]
    ).wait()
    hidden_store.wait()
    output_store.wait()
    grad_store.wait()


def body(
    n_dev,
    n_rep,
    n_y,
    n_core,
    features,
    history,
    new_owner,
    pull_rows,
    occupancy,
    adj_local,
    adj_boundary,
    w_first,
    bias_first,
    w_second,
    cotangent,
):
    rows, breadth = features.shape
    per_z = n_y * n_core
    slab = per_z * n_rep
    n_z = n_dev // per_z
    chunk = breadth // slab
    any_space = pl.BlockSpec(memory_space=pl.ANY)
    vmem = pl.BlockSpec(memory_space=pltpu.VMEM)
    wide = pltpu.VMEM((rows, breadth), BF16)
    square = pltpu.VMEM((rows, rows), BF16)
    hidden, output, grad = pl.pallas_call(
        functools.partial(step_kernel, n_dev, n_rep, n_y, n_core),
        name="gcn_step",
        out_shape=(
            jax.ShapeDtypeStruct((rows, breadth), BF16),
            jax.ShapeDtypeStruct((rows, breadth), BF16),
            jax.ShapeDtypeStruct((breadth, breadth), F32),
        ),
        in_specs=[any_space] * 2 + [vmem] * 3 + [any_space] * 3 + [vmem] + [any_space] * 2,
        out_specs=(any_space,) * 3,
        scratch_shapes=[
            wide,
            wide,
            square,
            square,
            square,
            pltpu.VMEM((breadth, breadth), BF16),
            pltpu.VMEM((breadth, breadth), BF16),
            wide,
            pltpu.VMEM((breadth, rows), BF16),
            wide,
            wide,
            wide,
            wide,
            pltpu.VMEM((n_dev, 1, 128), I32),
            pltpu.VMEM((n_dev, 128), I32),
            square,
            square,
            pltpu.VMEM((rows // 128, 2 * rows), F32),
            wide,
            wide,
            wide,
            wide,
            wide,
            wide,
            wide,
            wide,
            pltpu.VMEM((rows, breadth), F32),
            wide,
            wide,
            wide,
            pltpu.VMEM((breadth, breadth), F32),
            pltpu.VMEM((slab, chunk, breadth), F32),
            pltpu.VMEM((chunk, breadth), F32),
            pltpu.VMEM((n_z, chunk, breadth), F32),
            pltpu.VMEM((chunk, breadth), F32),
            pltpu.VMEM((breadth, breadth), F32),
            pltpu.SemaphoreType.DMA((7,)),
            pltpu.SemaphoreType.DMA((3,)),
            pltpu.SemaphoreType.DMA((10,)),
            pltpu.SemaphoreType.DMA((10,)),
        ],
        compiler_params=pltpu.CompilerParams(
            collective_id=0, has_side_effects=True, vmem_limit_bytes=60 * 2**20
        ),
    )(
        features,
        history,
        new_owner,
        pull_rows.reshape(rows // 128, 1, 128),
        occupancy,
        adj_local,
        adj_boundary,
        w_first,
        bias_first.reshape(1, breadth),
        w_second,
        cotangent,
    )
    return hidden, output, grad.T


def solution(mesh):
    split = P(("dev", "rep"), None)
    n_core, n_y = 2, 4
    return jax.shard_map(
        functools.partial(body, mesh.shape["dev"], mesh.shape["rep"], n_y, n_core),
        mesh=mesh,
        in_specs=(
            split,
            split,
            split,
            P(("dev", "rep")),
            split,
            split,
            split,
            P(),
            P(),
            P(),
            split,
        ),
        out_specs=(split, split, P()),
        check_vma=False,
    )
```

```python
import functools

import jax
import jax.numpy as jnp
from jax import lax
from jax.experimental import pallas as pl
from jax.experimental.pallas import tpu as pltpu
from jax.sharding import PartitionSpec as P

MESH = pl.DeviceIdType.MESH
F32, BF16, I32 = jnp.float32, jnp.bfloat16, jnp.int32

REQ, MIG_X, MIG_H, PULL_X, PUSH_1, PULL_H, PUSH_2, GRAD_A, GRAD_B, GRAD_C = range(10)


def iota(shape, dim):
    return lax.broadcasted_iota(I32, shape, dim)


def ones_where(condition):
    return jnp.where(condition, 1.0, 0.0).astype(BF16)


def dot(a, b):
    return jnp.dot(a, b, preferred_element_type=F32)


def step_kernel(
    n_dev,
    n_rep,
    n_y,
    n_core,
    features,
    history,
    new_owner,
    pull_rows,
    occupancy,
    adj_local,
    adj_boundary,
    w_first,
    bias,
    w_second,
    cotangent,
    hidden_out,
    output_out,
    grad_out,
    owner_ref,
    pull_ref,
    occ_ref,
    bias_first,
    x_in,
    h_in,
    local,
    edge,
    edge_t,
    w1,
    w2,
    cot,
    cot_t,
    far_cot_t,
    send_x,
    send_h,
    send_line,
    own_x,
    own_h,
    asked,
    asked_flat,
    sel,
    sel_t,
    occ_rows,
    fetch_x,
    fetch_h,
    part_1,
    part_2,
    far_x,
    far_h,
    push_1,
    push_2,
    acc,
    hidden,
    agg,
    result,
    grad,
    grad_sent,
    grad_in,
    slab_sum,
    line_in,
    total,
    line_sem,
    core_sem,
    load_sem,
    store_sem,
    send_sem,
    recv_sem,
):
    me, rep = lax.axis_index("dev"), lax.axis_index("rep")
    rows, breadth = x_in.shape
    per_peer = rows // n_dev
    per_z = n_y * n_core
    slab = per_z * n_rep
    n_z = n_dev // per_z
    chunk = breadth // slab
    my_z, my_yc = me // per_z, me % per_z
    my_slab = my_yc * n_rep + rep
    step = 256

    planes = [lax.rem(my_z + k, n_z) * per_z for k in range(n_z)]
    near_first = sorted(range(n_z), key=lambda k: (min(k, n_z - k), k))
    reps = [lax.rem(rep + k, n_rep) for k in range(n_rep)]

    def loop(low, high, visit):
        def run(i, carry):
            visit(i)
            return carry

        lax.fori_loop(low, high, run, 0)

    def each_on_line(visit):
        for k in near_first[1:]:
            visit(planes[k] + my_yc)

    def each_off_line(visit):
        def place(w):
            yc = lax.rem(my_yc + w, per_z)
            for k in near_first:
                visit(planes[k] + yc)

        loop(1, per_z, place)

    def each_peer(visit):
        each_on_line(visit)
        each_off_line(visit)

    def each_far_first(visit):
        def place(w):
            yc = lax.rem(my_yc + w, per_z)
            for k in near_first[::-1]:
                visit(planes[k] + yc)

        loop(1, per_z, place)
        for k in near_first[:0:-1]:
            visit(planes[k] + my_yc)

    def each_in_slab(visit):
        away = [(w, k) for w in range(per_z) for k in range(n_rep)]
        away.sort(key=lambda a: -min(a[0], per_z - a[0]) - n_core * min(a[1], n_rep - a[1]))
        places = [lax.rem(my_yc + w, per_z) for w in range(per_z)]
        for w, k in away[:-1]:
            visit(places[w], reps[k])

    loads = [
        pltpu.make_async_copy(src, dst, load_sem.at[k])
        for k, (src, dst) in enumerate(
            [
                (features, x_in),
                (history, h_in),
                (adj_local, local),
                (adj_boundary, edge),
                (cotangent, cot),
                (w_first, w1),
                (w_second, w2),
                (new_owner, owner_ref),
                (pull_rows, pull_ref),
                (occupancy, occ_ref),
                (bias, bias_first),
            ]
        )
    ]
    barrier = pltpu.get_barrier_semaphore()
    my_core = lax.rem(my_yc, n_core)
    along_y = [planes[0] + lax.rem(my_yc + k * n_core, per_z) for k in range(1, n_y)]
    other_core = planes[0] + my_yc + 1 - 2 * my_core

    def signal(semaphore, device):
        pl.semaphore_signal(semaphore, inc=1, device_id=device, device_id_type=MESH)

    for k in near_first[:0:-1]:
        signal(barrier, (planes[k] + my_yc, rep))
    for r in reps[1:]:
        signal(barrier, (me, r))
    for peer in along_y:
        signal(barrier, (peer, rep))
    signal(barrier, (other_core, rep))
    for k in (7, 0, 8, 1, 9, 2, 3, 4, 5, 6, 10):
        loads[k].start()

    loads[7].wait()
    owners = jnp.broadcast_to(owner_ref[...], (8, n_dev)).astype(F32).astype(BF16)
    spread = ones_where(iota((n_dev, rows), 0) == iota((n_dev, rows), 1) // per_peer)
    target = dot(owners, spread)[0:1].astype(I32) * per_peer + iota((1, rows), 1) % per_peer

    def arrange(src, dst):
        def run(i, carry):
            at = pl.ds(pl.multiple_of(i * step, step), step)
            pick = ones_where(iota((step, rows), 0) + i * step == target)
            dst[at] = dot(pick, src[...]).astype(BF16)
            return carry

        lax.fori_loop(0, rows // step, run, 0)

    loads[0].wait()
    arrange(x_in, send_x)

    def block(d):
        return pl.ds(pl.multiple_of(d * per_peer, per_peer), per_peer)

    own_x[block(me)] = send_x[block(me)]
    loads[8].wait()
    asked[me] = pull_ref[me // per_z]

    def remote(src, dst, stage, device):
        pltpu.make_async_remote_copy(
            src_ref=src,
            dst_ref=dst,
            send_sem=send_sem.at[stage],
            recv_sem=recv_sem.at[stage],
            device_id=device,
            device_id_type=MESH,
        ).start()

    def send_request(peer):
        remote(pull_ref.at[peer // per_z], asked.at[me], REQ, (peer, rep))

    def exchange(src, dst, stage, visit=each_peer):
        mine = block(me)
        visit(lambda peer: remote(src.at[block(peer)], dst.at[mine], stage, (peer, rep)))

    others = pl.ds(0, rows - per_peer)

    def landed(dst, stage):
        pltpu.make_async_copy(dst.at[others], dst.at[others], recv_sem.at[stage]).wait()

    def left(src, stage):
        pltpu.make_async_copy(src.at[others], src.at[others], send_sem.at[stage]).wait()

    pl.semaphore_wait(barrier, n_z - 1 + n_rep - 1 + n_y - 1 + 1)
    for peer in along_y:
        signal(line_sem, (peer, rep))
    each_on_line(send_request)
    exchange(send_x, own_x, MIG_X, each_on_line)

    loads[1].wait()
    row = iota((n_z * per_peer, rows), 0)
    line_row = (((my_z + row // per_peer) % n_z) * per_z + my_yc) * per_peer + row % per_peer
    send_line[...] = dot(ones_where(line_row == target), h_in[...]).astype(BF16)
    own_h[block(me)] = send_line[0:per_peer]
    for k in near_first[1:]:
        remote(
            send_line.at[pl.ds(k * per_peer, per_peer)],
            own_h.at[block(me)],
            MIG_H,
            (planes[k] + my_yc, rep),
        )
    pl.semaphore_wait(line_sem, n_y - 1)
    signal(core_sem, (other_core, rep))
    pl.semaphore_wait(core_sem, 1)
    each_off_line(send_request)
    exchange(send_x, own_x, MIG_X, each_off_line)
    arrange(h_in, send_h)
    exchange(send_h, own_h, MIG_H, each_off_line)

    n_tiles = 2 * rows // 128
    loads[9].wait()
    tile_of = ones_where(iota((n_tiles, 2 * rows), 0) == iota((n_tiles, 2 * rows), 1) // 128)
    occ_rows[...] = dot(occ_ref[...].astype(F32).astype(BF16), tile_of)
    loads[2].wait()
    loads[3].wait()

    def mask_rows(i, carry):
        at = pl.ds(pl.multiple_of(i * 128, 128), 128)
        there = occ_rows[pl.ds(i, 1), :]
        flags = jnp.broadcast_to(there, (128, 2 * rows)).astype(BF16)
        local[at] = local[at] * flags[:, :rows]
        kept = edge[at] * flags[:, rows:]
        edge[at] = kept
        edge_t[:, at] = kept.T
        return carry

    lax.fori_loop(0, rows // 128, mask_rows, 0)

    pltpu.make_async_copy(
        asked.at[pl.ds(0, n_dev - 1)], asked.at[pl.ds(0, n_dev - 1)], recv_sem.at[REQ]
    ).wait()
    for d in range(n_dev):
        asked_flat[d : d + 1, :] = asked[d]
    first = (me % per_z) * per_peer
    wanted = asked_flat[...]
    high = (wanted // per_peer).astype(F32).astype(BF16)
    low = (wanted % per_peer).astype(F32).astype(BF16)
    widen = ones_where(iota((128, rows), 0) == first + iota((128, rows), 1) % per_peer)
    along = dot(high, widen) * per_peer + dot(low, widen)
    mine = iota((n_dev, rows), 0) == iota((n_dev, rows), 1) // per_peer
    as_row = jnp.sum(jnp.where(mine, along, 0.0), axis=0, keepdims=True).astype(I32)
    all_ones = jnp.ones((128, 128), BF16)

    def select(i, carry):
        at = pl.ds(pl.multiple_of(i * step, step), step)
        sel[at] = ones_where(iota((step, rows), 0) + i * step == as_row)
        entry = iota((step, n_dev), 0) + i * step
        take = ones_where(entry // per_peer == iota((step, n_dev), 1))
        here = iota((step, 128), 1) == first + iota((step, 128), 0) % per_peer
        hi = jnp.where(here, dot(take, high), 0.0).astype(BF16)
        lo = jnp.where(here, dot(take, low), 0.0).astype(BF16)
        as_column = (dot(hi, all_ones) * per_peer + dot(lo, all_ones)).astype(I32)
        for c in range(rows // 128):
            sel_t[at, c * 128 : (c + 1) * 128] = ones_where(as_column == iota((step, 128), 1) + c * 128)
        return carry

    lax.fori_loop(0, rows // step, select, 0)

    def product(dst, a, b):
        def run(i, carry):
            at = pl.ds(pl.multiple_of(i * step, step), step)
            dst[at] = dot(a[at], b[...]).astype(dst.dtype)
            return carry

        lax.fori_loop(0, a.shape[0] // step, run, 0)

    def add_product(dst, a, b):
        def run(i, carry):
            at = pl.ds(pl.multiple_of(i * step, step), step)
            dst[at] += dot(a[at], b[...])
            return carry

        lax.fori_loop(0, a.shape[0] // step, run, 0)

    landed(own_x, MIG_X)
    product(fetch_x, sel_t, own_x)
    exchange(fetch_x, far_x, PULL_X)
    product(part_1, edge_t, own_x)
    exchange(part_1, push_1, PUSH_1)
    far_x[block(me)] = fetch_x[block(me)]
    push_1[block(me)] = part_1[block(me)]
    product(acc, local, own_x)

    landed(own_h, MIG_H)
    product(fetch_h, sel_t, own_h)
    exchange(fetch_h, far_h, PULL_H)
    far_h[block(me)] = fetch_h[block(me)]
    loads[4].wait()
    cot_t[...] = cot[...].T

    def pull_cot(i, carry):
        at = pl.ds(pl.multiple_of(i * step, step), step)
        far_cot_t[:, at] = dot(cot_t[...], sel[:, at]).astype(BF16)
        return carry

    lax.fori_loop(0, rows // step, pull_cot, 0)
    loads[5].wait()
    loads[6].wait()
    loads[10].wait()

    landed(far_x, PULL_X)
    add_product(acc, edge, far_x)
    landed(push_1, PUSH_1)

    def to_hidden(i, carry):
        at = pl.ds(pl.multiple_of(i * step, step), step)
        gathered = (acc[at] + dot(sel[at], push_1[...])).astype(BF16)
        hidden[at] = jnp.maximum(dot(gathered, w1[...]) + bias_first[...], 0.0).astype(BF16)
        return carry

    lax.fori_loop(0, rows // step, to_hidden, 0)

    product(part_2, edge_t, hidden)
    exchange(part_2, push_2, PUSH_2, each_far_first)
    push_2[block(me)] = part_2[block(me)]
    hidden_store = pltpu.make_async_copy(hidden, hidden_out, store_sem.at[0])
    hidden_store.start()
    product(acc, local, hidden)
    landed(far_h, PULL_H)
    add_product(acc, edge, far_h)
    agg[...] = acc[...].astype(BF16)
    grad[...] = dot(cot_t[...], agg[...])
    landed(push_2, PUSH_2)

    grad_sent[...] = grad[...] + dot(far_cot_t[...], push_2[...])

    def part_of(q):
        return pl.ds(pl.multiple_of(q * chunk, chunk), chunk)

    def scatter_grad(yc, r):
        q = yc * n_rep + r
        remote(grad_sent.at[part_of(q)], grad_in.at[my_slab], GRAD_A, (planes[0] + yc, r))

    each_in_slab(scatter_grad)
    grad_in[my_slab] = grad_sent[part_of(my_slab)]

    def to_output(i, carry):
        at = pl.ds(pl.multiple_of(i * step, step), step)
        gathered = (acc[at] + dot(sel[at], push_2[...])).astype(BF16)
        result[at] = dot(gathered, w2[...]).astype(BF16)
        return carry

    lax.fori_loop(0, rows // step, to_output, 0)
    output_store = pltpu.make_async_copy(result, output_out, store_sem.at[1])
    output_store.start()
    pltpu.make_async_copy(
        grad_in.at[pl.ds(0, slab - 1)], grad_in.at[pl.ds(0, slab - 1)], recv_sem.at[GRAD_A]
    ).wait()
    slab_sum[...] = jnp.sum(grad_in[...], axis=0)

    for k in near_first[:0:-1]:
        remote(slab_sum, line_in.at[my_z], GRAD_B, (planes[k] + my_yc, rep))
    line_in[my_z] = slab_sum[...]
    pltpu.make_async_copy(
        line_in.at[pl.ds(0, n_z - 1)], line_in.at[pl.ds(0, n_z - 1)], recv_sem.at[GRAD_B]
    ).wait()
    total[...] = jnp.sum(line_in[...], axis=0).astype(BF16)

    def spread_total(yc, r):
        remote(total, grad_out.at[part_of(my_slab)], GRAD_C, (planes[0] + yc, r))

    each_in_slab(spread_total)
    own_part = pltpu.make_async_copy(total, grad_out.at[part_of(my_slab)], store_sem.at[2])
    own_part.start()
    pltpu.make_async_copy(
        grad_out.at[pl.ds(0, breadth - chunk)],
        grad_out.at[pl.ds(0, breadth - chunk)],
        recv_sem.at[GRAD_C],
    ).wait()

    pltpu.make_async_copy(
        asked.at[pl.ds(0, n_dev - 1)], asked.at[pl.ds(0, n_dev - 1)], send_sem.at[REQ]
    ).wait()
    left(send_x, MIG_X)
    left(send_h, MIG_H)
    left(fetch_x, PULL_X)
    left(part_1, PUSH_1)
    left(fetch_h, PULL_H)
    left(part_2, PUSH_2)
    for stage, sent in ((GRAD_A, grad_sent), (GRAD_C, grad_out)):
        bulk = sent.at[pl.ds(0, breadth - chunk)]
        pltpu.make_async_copy(bulk, bulk, send_sem.at[stage]).wait()
    pltpu.make_async_copy(
        line_in.at[pl.ds(0, n_z - 1)], line_in.at[pl.ds(0, n_z - 1)], send_sem.at[GRAD_B]
    ).wait()
    hidden_store.wait()
    output_store.wait()
    own_part.wait()


def hand_over_kernel(hidden, output, grad, hidden_out, output_out, grad_out, a, b, c, d, in_sem, out_sem):
    loads = [
        pltpu.make_async_copy(src, dst, in_sem.at[k])
        for k, (src, dst) in enumerate([(grad, c), (hidden, a), (output, b)])
    ]
    stores = [
        pltpu.make_async_copy(src, dst, out_sem.at[k])
        for k, (src, dst) in enumerate([(d, grad_out), (a, hidden_out), (b, output_out)])
    ]
    for load in loads:
        load.start()
    for k in (1, 2):
        loads[k].wait()
        stores[k].start()
    loads[0].wait()
    d[...] = c[...].astype(F32).T
    stores[0].start()
    for store in stores:
        store.wait()


def body(
    n_dev,
    n_rep,
    n_y,
    n_core,
    features,
    history,
    new_owner,
    pull_rows,
    occupancy,
    adj_local,
    adj_boundary,
    w_first,
    bias_first,
    w_second,
    cotangent,
):
    rows, breadth = features.shape
    per_z = n_y * n_core
    slab = per_z * n_rep
    n_z = n_dev // per_z
    chunk = breadth // slab
    any_space = pl.BlockSpec(memory_space=pl.ANY)
    per_peer = rows // n_dev
    wide = pltpu.VMEM((rows, breadth), BF16)
    square = pltpu.VMEM((rows, rows), BF16)
    hidden, output, grad = pl.pallas_call(
        functools.partial(step_kernel, n_dev, n_rep, n_y, n_core),
        name="gcn_step",
        out_shape=(
            jax.ShapeDtypeStruct((rows, breadth), BF16),
            jax.ShapeDtypeStruct((rows, breadth), BF16),
            jax.ShapeDtypeStruct((breadth, breadth), BF16),
        ),
        in_specs=[any_space] * 11,
        out_specs=(any_space,) * 3,
        scratch_shapes=[
            pltpu.VMEM((1, n_dev), I32),
            pltpu.VMEM((rows // 128, 1, 128), I32),
            pltpu.VMEM((rows // 128, 2 * rows // 128), I32),
            pltpu.VMEM((1, breadth), F32),
            wide,
            wide,
            square,
            square,
            square,
            pltpu.VMEM((breadth, breadth), BF16),
            pltpu.VMEM((breadth, breadth), BF16),
            wide,
            pltpu.VMEM((breadth, rows), BF16),
            pltpu.VMEM((breadth, rows), BF16),
            wide,
            wide,
            pltpu.VMEM((n_z * per_peer, breadth), BF16),
            wide,
            wide,
            pltpu.VMEM((n_dev, 1, 128), I32),
            pltpu.VMEM((n_dev, 128), I32),
            square,
            square,
            pltpu.VMEM((rows // 128, 2 * rows), F32),
            wide,
            wide,
            wide,
            wide,
            wide,
            wide,
            wide,
            wide,
            pltpu.VMEM((rows, breadth), F32),
            wide,
            wide,
            wide,
            pltpu.VMEM((breadth, breadth), F32),
            pltpu.VMEM((breadth, breadth), F32),
            pltpu.VMEM((slab, chunk, breadth), F32),
            pltpu.VMEM((chunk, breadth), F32),
            pltpu.VMEM((n_z, chunk, breadth), F32),
            pltpu.VMEM((chunk, breadth), BF16),
            pltpu.SemaphoreType.REGULAR,
            pltpu.SemaphoreType.REGULAR,
            pltpu.SemaphoreType.DMA((11,)),
            pltpu.SemaphoreType.DMA((3,)),
            pltpu.SemaphoreType.DMA((10,)),
            pltpu.SemaphoreType.DMA((10,)),
        ],
        compiler_params=pltpu.CompilerParams(
            collective_id=0, has_side_effects=True, vmem_limit_bytes=60 * 2**20
        ),
    )(
        features,
        history,
        new_owner,
        pull_rows.reshape(rows // 128, 1, 128),
        occupancy,
        adj_local,
        adj_boundary,
        w_first,
        bias_first.reshape(1, breadth),
        w_second,
        cotangent,
    )
    return pl.pallas_call(
        hand_over_kernel,
        name="hand_over",
        out_shape=(
            jax.ShapeDtypeStruct((rows, breadth), BF16),
            jax.ShapeDtypeStruct((rows, breadth), BF16),
            jax.ShapeDtypeStruct((breadth, breadth), F32),
        ),
        in_specs=[any_space] * 3,
        out_specs=(any_space,) * 3,
        scratch_shapes=[
            wide,
            wide,
            pltpu.VMEM((breadth, breadth), BF16),
            pltpu.VMEM((breadth, breadth), F32),
            pltpu.SemaphoreType.DMA((3,)),
            pltpu.SemaphoreType.DMA((3,)),
        ],
        compiler_params=pltpu.CompilerParams(vmem_limit_bytes=60 * 2**20),
    )(hidden, output, grad)


def solution(mesh):
    split = P(("dev", "rep"), None)
    n_core, n_y = 2, 4
    return jax.shard_map(
        functools.partial(body, mesh.shape["dev"], mesh.shape["rep"], n_y, n_core),
        mesh=mesh,
        in_specs=(
            split,
            split,
            split,
            P(("dev", "rep")),
            split,
            split,
            split,
            P(),
            P(),
            P(),
            split,
        ),
        out_specs=(split, split, P()),
        check_vma=False,
    )
```
